32 devices in a mesh: dp: 16 (over z, y, core), cp: 2 (over x).
Axes of the slice: x: 2, y: 2, z: 4, core: 2. Of those that a mesh axis runs over, the one named last changes fastest.
Arguments:
- x_source: bfloat16 [16, 1024, 768], P(None, ('cp', 'dp')), may hold values from -6 to 6
- cotangent: bfloat16 [16, 1024, 768], P('dp', 'cp'), may hold values from -6 to 6
- lengths: int32 [16], replicated, may hold values from 1 to 1024, 10240 in all
- dealing: int32 [16], replicated, may hold values from 0 to 15, each once
- qkv_weight: float32 [768, 2304], P('cp', 'dp'), may hold values from -0.21875 to 0.21875
- proj_weight: float32 [768, 768], P('cp', 'dp'), may hold values from -2 to 2
- up_weight: float32 [768, 3072], P('cp', 'dp'), may hold values from -0.21875 to 0.21875
- down_weight: float32 [3072, 768], P('cp', 'dp'), may hold values from -0.109375 to 0.109375
- first_gain: float32 [768], P('dp'), may hold values from 0.1 to 1.9
- first_shift: float32 [768], P('dp'), may hold values from -1.75 to 1.75
- proj_bias: float32 [768], P('dp'), may hold values from -1.75 to 1.75
- second_gain: float32 [768], P('dp'), may hold values from 0.1 to 1.9
- second_shift: float32 [768], P('dp'), may hold values from -1.75 to 1.75
- up_bias: float32 [3072], P('dp'), may hold values from -3 to 3
- down_bias: float32 [768], P('dp'), may hold values from -1.75 to 1.75
Outputs:
- output: bfloat16 [16, 1024, 768], P('dp', 'cp')
- input_grad: bfloat16 [16, 1024, 768], P(None, ('cp', 'dp'))
- qkv_grad: float32 [768, 2304], P('cp', 'dp')
- proj_grad: float32 [768, 768], P('cp', 'dp')
- up_grad: float32 [768, 3072], P('cp', 'dp')
- down_grad: float32 [3072, 768], P('cp', 'dp')
- first_gain_grad: float32 [768], P('dp')
- first_shift_grad: float32 [768], P('dp')
- proj_bias_grad: float32 [768], P('dp')
- second_gain_grad: float32 [768], P('dp')
- second_shift_grad: float32 [768], P('dp')
- up_bias_grad: float32 [3072], P('dp')
- down_bias_grad: float32 [768], P('dp')
The draws below stay inside these ranges and needn't reach their ends.
Inputs may be any that keep to these rules, and one draw needn't show every extreme that they name: The lengths sum to 10240 and the longest is exactly 1024. `dealing`: a permutation of the sequence numbers.
All inputs are finite; a program needn't handle non-finite values.
Results may differ from the reference program's by a relative error of at most 0.019.
Values may be sent and summed in bfloat16 or wider, within the bound.
A program may use at most 192 MiB of HBM per device.

```python
import math
import jax
import jax.numpy as jnp
import numpy as np
from jax import lax

D = 768
HEADS = 12
HEAD_DIM = 64
FF = 3072
LEN = 1024
SEQS = 16


def block_scale(rng, shape, split, low, largest):
    level, own = 1.0, jax.random.fold_in(rng, 6)
    for dim, parts in split:
        steps = jnp.exp(jax.random.uniform(jax.random.fold_in(own, dim), (parts,), jnp.float32, low / len(split), largest / len(split)))
        level = level * jnp.repeat(steps, shape[dim] // parts).reshape([-1 if axis == dim else 1 for axis in range(len(shape))])
    return level


def length_profile(count, total, limit, skew):
    weights = [(1 << 20) // math.isqrt(grade ** skew) + 1 for grade in range(2, count + 1)]
    spare, holding = total - limit - (count - 1), [1] * (count - 1)
    while spare > 0:
        free = [i for i in range(count - 1) if holding[i] < limit]
        whole, remaining = sum([weights[i] for i in free]), spare
        for i in free:
            more = min(limit - holding[i], max(1, remaining * weights[i] // whole), spare)
            holding[i] = holding[i] + more
            spare = spare - more
    return np.array([limit] + holding)


def ragged(key, count, total, bound, slope):
    if count == 2:
        one = jax.random.randint(key, (), max(1, total - bound), min(bound, total - 1) + 1)
        return jnp.stack([one, total - one])
    tallies = jnp.asarray(length_profile(count, total, bound, slope), jnp.int32)
    couples = (count - 1) // 2
    giver, receiver = tallies[1:1 + 2 * couples:2], tallies[2:2 + 2 * couples:2]
    margin = jnp.minimum(giver - 1, bound - receiver)
    moved = jax.random.randint(jax.random.fold_in(key, 1), (couples,), 0, 1 << 20) % (margin + 1)
    tallies = tallies.at[1:1 + 2 * couples:2].set(giver - moved).at[2:2 + 2 * couples:2].set(receiver + moved)
    return tallies[jax.random.permutation(jax.random.fold_in(key, 2), count)]


def bell_draw(key, extent, scale, limit, shards=(), held_as=jnp.bfloat16):
    values = jax.random.normal(key, extent, jnp.float32) * scale
    if len(shards) > 0:
        values = block_scale(key, extent, shards, -0.22, 0.18) * values
    return jnp.clip(values, min=-limit, max=limit).astype(held_as)


def setup_inputs(seed: int = 0) -> dict:
    streams_of = jax.random.split(jax.random.key(seed), 16)
    x_source = bell_draw(streams_of[0], (SEQS, LEN, D), 1.0, 6.0, ((1, 32),))
    cotangent = bell_draw(streams_of[1], (SEQS, LEN, D), 1.0, 6.0, ((0, 16), (1, 2)))
    lengths = ragged(streams_of[2], SEQS, SEQS * LEN * 5 // 8, LEN, 1).astype(jnp.int32)
    dealing = jax.random.permutation(streams_of[3], SEQS).astype(jnp.int32)
    qkv_weight = bell_draw(streams_of[4], (D, 3 * D), D ** -0.5, 0.21875, ((0, 2), (1, 16)), jnp.float32)
    proj_weight = bell_draw(streams_of[5], (D, D), (max(1, D // 100)) ** -0.5, 2.0, ((0, 2), (1, 16)), jnp.float32)
    up_weight = bell_draw(streams_of[6], (D, FF), D ** -0.5, 0.21875, ((0, 2), (1, 16)), jnp.float32)
    down_weight = bell_draw(streams_of[7], (FF, D), FF ** -0.5, 0.109375, ((0, 2), (1, 16)), jnp.float32)
    first_gain = jnp.clip(1.0 + 0.18 * jax.random.normal(streams_of[8], (D,), jnp.float32), 0.1, 1.9)
    first_shift = bell_draw(streams_of[9], (D,), 0.3, 1.75, ((0, 16),), jnp.float32)
    proj_bias = bell_draw(streams_of[10], (D,), 0.3, 1.75, ((0, 16),), jnp.float32)
    second_gain = jnp.clip(1.0 + 0.18 * jax.random.normal(streams_of[11], (D,), jnp.float32), 0.1, 1.9)
    second_shift = bell_draw(streams_of[12], (D,), 0.3, 1.75, ((0, 16),), jnp.float32)
    up_bias = bell_draw(streams_of[13], (FF,), 0.5, 3.0, ((0, 16),), jnp.float32)
    down_bias = bell_draw(streams_of[14], (D,), 0.3, 1.75, ((0, 16),), jnp.float32)
    return dict(x_source=x_source, cotangent=cotangent, lengths=lengths, dealing=dealing, qkv_weight=qkv_weight, proj_weight=proj_weight, up_weight=up_weight, down_weight=down_weight, first_gain=first_gain, first_shift=first_shift, proj_bias=proj_bias, second_gain=second_gain, second_shift=second_shift, up_bias=up_bias, down_bias=down_bias)


EPSILON = 1e-05
NEG_BIG = -1e+30
TANH_SCALE = 0.7978845608028654
CUBIC_TERM = 0.044715

@jax.custom_vjp
def low(v):
    return lax.optimization_barrier(v.astype(jnp.bfloat16)).astype(jnp.float32)

@jax.custom_vjp
def low_back(v):
    return v

def low_keep(v):
    return (low(v), None)

def low_pass(kept, grad):
    return (grad,)

def back_keep(v):
    return (v, None)

def back_low(kept, grad):
    return (low(grad),)
low.defvjp(low_keep, low_pass)
low_back.defvjp(back_keep, back_low)

def layer_norm(values, scaling, offset):
    centered = values - lax.optimization_barrier(jnp.mean(values, axis=-1, keepdims=True))
    spread = lax.optimization_barrier(jnp.mean(centered * centered, axis=-1, keepdims=True))
    return centered * lax.rsqrt(spread + EPSILON) * scaling + offset

def gelu_tanh(values):
    return 0.5 * values * (1.0 + jnp.tanh(TANH_SCALE * (values + CUBIC_TERM * values * values * values)))

def block_forward(inputs, length, qkv_weight, proj_weight, up_weight, down_weight, first_gain, first_shift, proj_bias, second_gain, second_shift, up_bias, down_bias):
    highest = lax.Precision.HIGHEST
    row_count = inputs.shape[0]
    act_one = low(layer_norm(inputs, low(first_gain), low(first_shift)))
    mixed_rows = low_back(low(jnp.dot(act_one, low(qkv_weight), precision=highest)))
    queries = mixed_rows[:, :D].reshape(row_count, HEADS, HEAD_DIM)
    key_rows = mixed_rows[:, D:2 * D].reshape(row_count, HEADS, HEAD_DIM)
    val_rows = mixed_rows[:, 2 * D:].reshape(row_count, HEADS, HEAD_DIM)
    scores = jnp.einsum('qhd,khd->hqk', queries, key_rows, precision=highest) * HEAD_DIM ** (-0.5)
    places = jnp.arange(row_count)
    scores = low_back(jnp.where(places[None, :] <= places[:, None], scores, NEG_BIG))
    row_top = lax.optimization_barrier(jnp.max(scores, axis=-1, keepdims=True))
    exponent = jnp.exp(scores - row_top)
    weights = exponent / lax.optimization_barrier(jnp.sum(exponent, axis=-1, keepdims=True))
    attended = jnp.einsum('hqk,khd->qhd', low(weights), val_rows, precision=highest).reshape(row_count, D)
    attended = low_back(low(attended))
    residual = inputs + low_back(jnp.dot(attended, low(proj_weight), precision=highest)) + low(proj_bias)
    act_two = low(layer_norm(residual, low(second_gain), low(second_shift)))
    up_raw = low_back(jnp.dot(act_two, low(up_weight), precision=highest) + low(up_bias))
    hidden = low(gelu_tanh(up_raw))
    result = residual + jnp.dot(hidden, low(down_weight), precision=highest) + low(down_bias)
    return jnp.where(places[:, None] < length, result, 0.0)

def reference(x_source, cotangent, lengths, dealing, qkv_weight, proj_weight, up_weight, down_weight, first_gain, first_shift, proj_bias, second_gain, second_shift, up_bias, down_bias):
    owners = jnp.argsort(dealing).astype(jnp.int32)
    x_slots = x_source[owners]
    len_slots = lengths[owners]
    params = (qkv_weight, proj_weight, up_weight, down_weight, first_gain, first_shift, proj_bias, second_gain, second_shift, up_bias, down_bias)

    def one_sequence(totals, item):
        x_one, length, grad_one = item
        result, back = jax.vjp(lambda inputs, *weights: block_forward(inputs, length, *weights), x_one.astype(jnp.float32), *params)
        grads = back(grad_one.astype(jnp.float32))
        totals = tuple((former + latter for former, latter in zip(totals, grads[1:])))
        return (totals, (result.astype(jnp.bfloat16), grads[0].astype(jnp.bfloat16)))
    zeros = tuple((jnp.zeros_like(param) for param in params))
    totals, (output, grad_slots) = lax.scan(one_sequence, zeros, (x_slots, len_slots, cotangent))
    input_grad = grad_slots[dealing]
    return (output, input_grad, totals[0], totals[1], totals[2], totals[3], totals[4], totals[5], totals[6], totals[7], totals[8], totals[9], totals[10])
```

```python
import functools
import math

import jax
import jax.numpy as jnp
from jax import lax
from jax.experimental import pallas as pl
from jax.experimental.pallas import tpu as pltpu
from jax.sharding import PartitionSpec as P

MESH = pl.DeviceIdType.MESH

HEADS = 12
HEAD_DIM = 64


EPSILON = 1e-05
NEG_BIG = -1e30
TANH_SCALE = 0.7978845608028654
CUBIC_TERM = 0.044715


def layer_norm(values, scaling, offset):
    centered = values - jnp.mean(values, axis=-1, keepdims=True)
    spread = jnp.mean(centered * centered, axis=-1, keepdims=True)
    return centered * lax.rsqrt(spread + EPSILON) * scaling + offset


def gelu_tanh(values):
    return (
        0.5
        * values
        * (1.0 + jnp.tanh(TANH_SCALE * (values + CUBIC_TERM * values * values * values)))
    )


def grouped(array, block_seqs):
    return array.reshape(
        (array.shape[0] // block_seqs, block_seqs, array.shape[1], HEADS, array.shape[2] // HEADS)
    )


def grouped_stats(array, block_seqs):
    return array.reshape((array.shape[0] // block_seqs, block_seqs) + array.shape[1:])


def joined(array):
    return array.reshape(
        (array.shape[0] * array.shape[1], array.shape[2], array.shape[3] * array.shape[4])
    )


def masked_scores(queries, key_rows, query_start, score_scale):
    scores = (
        jnp.einsum("bqhd,bkhd->bhqk", queries, key_rows, preferred_element_type=jnp.float32)
        * score_scale
    )
    query_pos = query_start + jnp.arange(queries.shape[1])
    key_pos = jnp.arange(key_rows.shape[1])
    return jnp.where(key_pos[None, :] <= query_pos[:, None], scores, NEG_BIG)


def attend(inputs, query_start, score_scale):
    queries, key_rows, val_rows = inputs
    scores = masked_scores(queries, key_rows, query_start, score_scale)
    row_top = jnp.max(scores, axis=-1, keepdims=True)
    exponent = jnp.exp(scores - row_top)
    totals = jnp.sum(exponent, axis=-1, keepdims=True)
    weights = (exponent / totals).astype(jnp.bfloat16)
    attended = jnp.einsum("bhqk,bkhd->bqhd", weights, val_rows, preferred_element_type=jnp.float32)
    return (attended.astype(jnp.bfloat16), (row_top + jnp.log(totals))[..., 0])


def rows_back(inputs, query_start, score_scale):
    queries, key_rows, val_rows, grad_rows, log_total = inputs
    scores = masked_scores(queries, key_rows, query_start, score_scale)
    weights = jnp.exp(scores - log_total[..., None])
    grad_weights = jnp.einsum(
        "bqhd,bkhd->bhqk", grad_rows, val_rows, preferred_element_type=jnp.float32
    )
    delta_rows = jnp.sum(weights * grad_weights, axis=-1)
    grad_scores = (weights * (grad_weights - delta_rows[..., None])).astype(jnp.bfloat16)
    grad_query = (
        jnp.einsum("bhqk,bkhd->bqhd", grad_scores, key_rows, preferred_element_type=jnp.float32)
        * score_scale
    )
    grad_keys = (
        jnp.einsum("bhqk,bqhd->bkhd", grad_scores, queries, preferred_element_type=jnp.float32)
        * score_scale
    )
    grad_vals = jnp.einsum(
        "bhqk,bqhd->bkhd",
        weights.astype(jnp.bfloat16),
        grad_rows,
        preferred_element_type=jnp.float32,
    )
    return (grad_query, grad_keys, grad_vals)


def fetch_weights(
    qkv_weight,
    proj_weight,
    up_weight,
    down_weight,
    first_gain,
    first_shift,
    proj_bias,
    second_gain,
    second_shift,
    up_bias,
    down_bias,
):
    qkv_part, proj_part, up_part, down_part = (
        lax.all_gather(qkv_weight.astype(jnp.bfloat16), "cp", axis=0, tiled=True),
        lax.all_gather(proj_weight.astype(jnp.bfloat16), "cp", axis=0, tiled=True),
        lax.all_gather(up_weight.astype(jnp.bfloat16), "cp", axis=0, tiled=True),
        lax.all_gather(down_weight.astype(jnp.bfloat16), "cp", axis=0, tiled=True),
    )
    return (
        lax.all_gather(qkv_part, "dp", axis=1, tiled=True),
        lax.all_gather(proj_part, "dp", axis=1, tiled=True),
        lax.all_gather(up_part, "dp", axis=1, tiled=True),
        lax.all_gather(down_part, "dp", axis=1, tiled=True),
        lax.all_gather(first_gain.astype(jnp.bfloat16), "dp", axis=0, tiled=True),
        lax.all_gather(first_shift.astype(jnp.bfloat16), "dp", axis=0, tiled=True),
        lax.all_gather(proj_bias.astype(jnp.bfloat16), "dp", axis=0, tiled=True),
        lax.all_gather(second_gain.astype(jnp.bfloat16), "dp", axis=0, tiled=True),
        lax.all_gather(second_shift.astype(jnp.bfloat16), "dp", axis=0, tiled=True),
        lax.all_gather(up_bias.astype(jnp.bfloat16), "dp", axis=0, tiled=True),
        lax.all_gather(down_bias.astype(jnp.bfloat16), "dp", axis=0, tiled=True),
    )


def mat_rows(left, right):
    return jnp.einsum("sqd,de->sqe", left, right, preferred_element_type=jnp.float32)


def mat_back(left, right):
    return jnp.einsum("sqe,de->sqd", left, right, preferred_element_type=jnp.float32)


def mat_grad(left, right):
    return jnp.einsum("sqd,sqe->de", left, right, preferred_element_type=jnp.float32)


def local(
    x_source,
    cotangent,
    lengths,
    dealing,
    qkv_weight,
    proj_weight,
    up_weight,
    down_weight,
    first_gain,
    first_shift,
    proj_bias,
    second_gain,
    second_shift,
    up_bias,
    down_bias,
):
    groups = lax.axis_size("dp")
    seqs_all, piece_rows, features = x_source.shape
    seq_group = seqs_all // groups
    span_rows = groups * piece_rows
    score_scale = HEAD_DIM ** (-0.5)
    block_seqs = math.gcd(seq_group, max(1, 512 // span_rows))
    owners = jnp.argsort(dealing)
    send_order = owners.reshape(groups, seq_group).T.reshape(-1)
    outgoing = x_source[send_order].reshape(seq_group, span_rows, features)
    arrived = lax.all_to_all(outgoing, "dp", split_axis=1, concat_axis=1, tiled=True)
    first_slot = lax.axis_index("dp") * seq_group
    my_lengths = lax.dynamic_slice_in_dim(lengths[owners], first_slot, seq_group)
    query_start = lax.axis_index("cp") * span_rows
    positions = query_start + jnp.arange(span_rows)
    live_rows = positions[None, :] < my_lengths[:, None]
    fetched = fetch_weights(
        qkv_weight,
        proj_weight,
        up_weight,
        down_weight,
        first_gain,
        first_shift,
        proj_bias,
        second_gain,
        second_shift,
        up_bias,
        down_bias,
    )
    qkv_full, proj_full, up_full, down_full = (fetched[0], fetched[1], fetched[2], fetched[3])
    gain_one, shift_one, bias_proj, gain_two, shift_two, bias_up, bias_down = [
        vector.astype(jnp.float32) for vector in fetched[4:]
    ]
    inputs_f = arrived.astype(jnp.float32)
    norm_one, back_one = jax.vjp(layer_norm, inputs_f, gain_one, shift_one)
    act_one = norm_one.astype(jnp.bfloat16)
    mixed_rows = mat_rows(act_one, qkv_full).astype(jnp.bfloat16)
    queries = mixed_rows[..., :features]
    kv_local = mixed_rows[..., features:]
    kv_all = lax.all_gather(kv_local, "cp", axis=1, tiled=True)
    attended, log_total = lax.map(
        lambda inputs: attend(inputs, query_start, score_scale),
        (
            grouped(queries, block_seqs),
            grouped(kv_all[..., :features], block_seqs),
            grouped(kv_all[..., features:], block_seqs),
        ),
    )
    attended = joined(attended)
    log_total = log_total.reshape((seq_group,) + log_total.shape[2:])
    residual = inputs_f + mat_rows(attended, proj_full) + bias_proj
    norm_two, back_two = jax.vjp(layer_norm, residual, gain_two, shift_two)
    act_two = norm_two.astype(jnp.bfloat16)
    up_raw = mat_rows(act_two, up_full) + bias_up
    hidden, back_gelu = jax.vjp(gelu_tanh, up_raw)
    hid_low = hidden.astype(jnp.bfloat16)
    result = residual + mat_rows(hid_low, down_full) + bias_down
    output = jnp.where(live_rows[..., None], result, 0.0).astype(jnp.bfloat16)
    fetched = fetch_weights(
        qkv_weight,
        proj_weight,
        up_weight,
        down_weight,
        first_gain,
        first_shift,
        proj_bias,
        second_gain,
        second_shift,
        up_bias,
        down_bias,
    )
    qkv_full, proj_full, up_full, down_full = (fetched[0], fetched[1], fetched[2], fetched[3])
    gain_one, gain_two = (fetched[4].astype(jnp.float32), fetched[7].astype(jnp.float32))
    grad_out = jnp.where(live_rows[..., None], cotangent.astype(jnp.float32), 0.0)
    grad_low = grad_out.astype(jnp.bfloat16)
    grad_down = mat_grad(hid_low, grad_low)
    grad_bias_down = jnp.sum(grad_out, axis=(0, 1))
    grad_hidden = mat_back(grad_low, down_full)
    grad_up_raw = back_gelu(grad_hidden)[0].astype(jnp.bfloat16)
    grad_up = mat_grad(act_two, grad_up_raw)
    grad_bias_up = jnp.sum(grad_up_raw.astype(jnp.float32), axis=(0, 1))
    grad_act_two = mat_back(grad_up_raw, up_full)
    grad_resid, grad_gain_two, grad_shift_two = back_two(grad_act_two)
    grad_resid = grad_resid + grad_out
    grad_bias_proj = jnp.sum(grad_resid, axis=(0, 1))
    resid_low = grad_resid.astype(jnp.bfloat16)
    grad_proj = mat_grad(attended, resid_low)
    grad_attended = mat_back(resid_low, proj_full).astype(jnp.bfloat16)
    kv_back = lax.all_gather(kv_local, "cp", axis=1, tiled=True)
    key_rows = kv_back[..., :features]
    val_rows = kv_back[..., features:]
    grad_query, grad_keys, grad_vals = lax.map(
        lambda inputs: rows_back(inputs, query_start, score_scale),
        (
            grouped(queries, block_seqs),
            grouped(key_rows, block_seqs),
            grouped(val_rows, block_seqs),
            grouped(grad_attended, block_seqs),
            grouped_stats(log_total, block_seqs),
        ),
    )
    grad_keys, grad_vals = (
        lax.psum_scatter(
            joined(grad_keys).astype(jnp.bfloat16), "cp", scatter_dimension=1, tiled=True
        ).astype(jnp.float32),
        lax.psum_scatter(
            joined(grad_vals).astype(jnp.bfloat16), "cp", scatter_dimension=1, tiled=True
        ).astype(jnp.float32),
    )
    grad_mixed = jnp.concatenate([joined(grad_query), grad_keys, grad_vals], axis=-1).astype(
        jnp.bfloat16
    )
    grad_qkv = mat_grad(act_one, grad_mixed)
    grad_act_one = mat_back(grad_mixed, qkv_full)
    grad_input, grad_gain_one, grad_shift_one = back_one(grad_act_one)
    grad_input = (grad_input + grad_resid).astype(jnp.bfloat16)
    returned = lax.all_to_all(grad_input, "dp", split_axis=1, concat_axis=0, tiled=True)
    input_grad = returned[dealing]
    (
        grad_qkv,
        grad_proj,
        grad_up,
        grad_down,
        grad_gain_one,
        grad_shift_one,
        grad_bias_proj,
        grad_gain_two,
        grad_shift_two,
        grad_bias_up,
        grad_bias_down,
    ) = (
        lax.psum_scatter(
            grad_qkv.astype(jnp.bfloat16), "dp", scatter_dimension=1, tiled=True
        ).astype(jnp.float32),
        lax.psum_scatter(
            grad_proj.astype(jnp.bfloat16), "dp", scatter_dimension=1, tiled=True
        ).astype(jnp.float32),
        lax.psum_scatter(
            grad_up.astype(jnp.bfloat16), "dp", scatter_dimension=1, tiled=True
        ).astype(jnp.float32),
        lax.psum_scatter(
            grad_down.astype(jnp.bfloat16), "dp", scatter_dimension=1, tiled=True
        ).astype(jnp.float32),
        lax.psum_scatter(
            grad_gain_one.astype(jnp.bfloat16), "dp", scatter_dimension=0, tiled=True
        ).astype(jnp.float32),
        lax.psum_scatter(
            grad_shift_one.astype(jnp.bfloat16), "dp", scatter_dimension=0, tiled=True
        ).astype(jnp.float32),
        lax.psum_scatter(
            grad_bias_proj.astype(jnp.bfloat16), "dp", scatter_dimension=0, tiled=True
        ).astype(jnp.float32),
        lax.psum_scatter(
            grad_gain_two.astype(jnp.bfloat16), "dp", scatter_dimension=0, tiled=True
        ).astype(jnp.float32),
        lax.psum_scatter(
            grad_shift_two.astype(jnp.bfloat16), "dp", scatter_dimension=0, tiled=True
        ).astype(jnp.float32),
        lax.psum_scatter(
            grad_bias_up.astype(jnp.bfloat16), "dp", scatter_dimension=0, tiled=True
        ).astype(jnp.float32),
        lax.psum_scatter(
            grad_bias_down.astype(jnp.bfloat16), "dp", scatter_dimension=0, tiled=True
        ).astype(jnp.float32),
    )
    grad_qkv, grad_proj, grad_up, grad_down = (
        lax.psum_scatter(
            grad_qkv.astype(jnp.bfloat16), "cp", scatter_dimension=0, tiled=True
        ).astype(jnp.float32),
        lax.psum_scatter(
            grad_proj.astype(jnp.bfloat16), "cp", scatter_dimension=0, tiled=True
        ).astype(jnp.float32),
        lax.psum_scatter(
            grad_up.astype(jnp.bfloat16), "cp", scatter_dimension=0, tiled=True
        ).astype(jnp.float32),
        lax.psum_scatter(
            grad_down.astype(jnp.bfloat16), "cp", scatter_dimension=0, tiled=True
        ).astype(jnp.float32),
    )
    (
        grad_gain_one,
        grad_shift_one,
        grad_bias_proj,
        grad_gain_two,
        grad_shift_two,
        grad_bias_up,
        grad_bias_down,
    ) = lax.psum(
        (
            grad_gain_one,
            grad_shift_one,
            grad_bias_proj,
            grad_gain_two,
            grad_shift_two,
            grad_bias_up,
            grad_bias_down,
        ),
        "cp",
    )
    return (
        output,
        input_grad,
        grad_qkv,
        grad_proj,
        grad_up,
        grad_down,
        grad_gain_one,
        grad_shift_one,
        grad_bias_proj,
        grad_gain_two,
        grad_shift_two,
        grad_bias_up,
        grad_bias_down,
    )


BF16 = jnp.bfloat16
F32 = jnp.float32
ROWS = 512
QUARTER = 256
WIDE = 768
HIDDEN = 3072
PIECE = 32
SHARDS = ((144, 384), (48, 384), (192, 384), (48, 1536))
QKV, PROJ, UP, DOWN = range(4)
G1, C1, BP, G2, C2, BD, BU = range(7)


def fits_block(mesh):
    return mesh.shape["dp"] == 16 and mesh.shape["cp"] == 2


def dot_nt(left, right):
    return lax.dot_general(left, right, (((1,), (1,)), ((), ())), preferred_element_type=F32)


def dot_nn(left, right):
    return lax.dot_general(left, right, (((1,), (0,)), ((), ())), preferred_element_type=F32)


def dot_tn(left, right):
    return lax.dot_general(left, right, (((0,), (0,)), ((), ())), preferred_element_type=F32)


def block_kernel(
    length_ref,
    xg,
    cot,
    wq_in,
    wp_in,
    wu_in,
    wd_in,
    vec_in,
    out_ref,
    ret_ref,
    gq_out,
    gp_out,
    gu_out,
    gd_out,
    gvec_out,
    wq,
    wp,
    wu,
    wd,
    gq,
    r0_refs,
    r1_refs,
    r2_refs,
    r3_refs,
    acts,
    sems,
):
    X, A1, M, KVP, O, R, A2, HD, DU, T1, DRR, G, GT, DKVP, RK, LSE, VEC, VF, CS, VGS, VGR = acts
    (
        x_s,
        x_r,
        v_s,
        v_r,
        c_s,
        c_r,
        zs,
        n1s,
        n2s,
        ps,
        rsem,
        prsem,
        kv_s,
        kv_r,
        o_s,
        o_r,
        r0s,
        r0r,
        r1s,
        r1r,
        r2s,
        r2r,
        r3s,
        r3r,
        dk_s,
        dk_r,
        ret_s,
        ret_r,
        vg_s,
        vg_r,
    ) = sems
    w_refs = (wq, wp, wu, wd)
    w_in = (wq_in, wp_in, wu_in, wd_in)
    grads = (gq, wp, wu, wd)
    g_out = (gq_out, gp_out, gu_out, gd_out)

    dp = lax.axis_index("dp")
    x = lax.axis_index("cp")
    z = lax.div(dp, 4)
    y = lax.rem(lax.div(dp, 2), 2)
    c = lax.rem(dp, 2)
    slot = z * 4 + y * 2 + x
    x1, y1 = x + (1 - c) * (1 - 2 * x), y + c * (1 - 2 * y)
    x2, y2 = x + c * (1 - 2 * x), y + (1 - c) * (1 - 2 * y)

    def dev(zt, yt, ct, xt):
        return (zt * 4 + yt * 2 + ct, xt)

    partner = dev(z, y, 1 - c, x)
    near_one = dev(z, y1, c, x1)
    near_two = dev(z, y2, c, x2)

    def remote(src, dst, send, recv, target):
        return pltpu.make_async_remote_copy(
            src_ref=src,
            dst_ref=dst,
            send_sem=send,
            recv_sem=recv,
            device_id=target,
            device_id_type=MESH,
        )

    def loop(count, body, start=0):
        def step(k, carry):
            body(k)
            return carry

        lax.fori_loop(start, count, step, 0)

    def rows_at(at, count, multiple):
        return pl.ds(pl.multiple_of(at, multiple), count)

    barrier = pltpu.get_barrier_semaphore()
    me = dp * 2 + x

    def greet(k):
        other = lax.rem(me + k, 32)
        pl.semaphore_signal(
            barrier,
            inc=1,
            device_id=(lax.div(other, 2), lax.rem(other, 2)),
            device_id_type=MESH,
        )

    loop(32, greet, 1)
    pl.semaphore_wait(barrier, 31)

    piece = lax.rem(dp, 8)
    x_core = lax.rem(x + lax.div(z, 2), 2)
    x_rows = X.at[rows_at(x * QUARTER + piece * PIECE, PIECE, PIECE), :]
    x_mine = x_core == c

    def x_copy(k):
        to = lax.rem(slot + k, 16)
        target = dev(lax.div(to, 4), lax.rem(lax.div(to, 2), 2), x_core, lax.rem(to, 2))
        return remote(xg.at[to], x_rows, x_s.at[k], x_r.at[x * 8 + piece], target)

    def x_local():
        return pltpu.make_async_copy(xg.at[slot], x_rows, x_r.at[x * 8 + piece])

    @pl.when(x_mine)
    def _():
        x_local().start()

    @pl.when(jnp.logical_not(x_mine))
    def _():
        x_copy(0).start()

    loop(16, lambda k: x_copy(k).start(), 1)

    def v_copy(k):
        to = lax.rem(dp + k, 16)
        return remote(vec_in, VEC.at[dp], v_s.at[k], v_r.at[dp], (to, x))

    loop(16, lambda k: v_copy(k).start(), 1)
    VEC[pl.ds(dp, 1)] = vec_in[...][None]

    def ident(zt, yt, xt):
        return zt * 4 + yt * 2 + xt

    def shard(ref, m, zt, yt, ct, xt):
        n, lanes = SHARDS[m]
        return ref.at[
            rows_at((zt * 4 + yt * 2 + ct) * n, n, 16), rows_at(xt * lanes, lanes, 128)
        ]

    def put_own(m):
        n, lanes = SHARDS[m]
        w_refs[m][rows_at(dp * n, n, 16), rows_at(x * lanes, lanes, 128)] = w_in[m][...]

    def z_copy(m, k):
        target = dev(lax.rem(z + k, 4), y, c, x)
        return remote(
            w_in[m],
            shard(w_refs[m], m, z, y, c, x),
            zs.at[m, k],
            rsem.at[m, ident(z, y, x)],
            target,
        )

    def pass_on(m, first, zt, yt, xt, send, recv, target):
        place = shard(w_refs[m], m, zt, yt, c, xt)
        return remote(w_in[m] if first else place, place, send, recv, target)

    def arrived(m, zt, yt, xt):
        place = shard(w_refs[m], m, zt, yt, c, xt)
        remote(place, place, zs.at[m, 0], rsem.at[m, ident(zt, yt, xt)], partner).wait_recv()

    def send_one(m, first, k):
        zt = lax.rem(z + k, 4)
        return pass_on(
            m, first, zt, y, x, n1s.at[m, k], rsem.at[m, ident(zt, y, x)], near_one
        )

    def send_two(m, first, k):
        zt, yt, xt = (lax.rem(z + k, 4), y, x)
        return pass_on(
            m, first, zt, yt, xt, n2s.at[m, k], rsem.at[m, ident(zt, yt, xt)], near_two
        )

    def send_two_late(m, k):
        zt = lax.rem(z + k, 4)
        return pass_on(
            m, False, zt, y1, x1, n2s.at[m, 4 + k], rsem.at[m, ident(zt, y1, x1)], near_two
        )

    def far_place(k):
        late = lax.div(k, 4)
        zt = lax.rem(z + lax.rem(k, 4), 4)
        yt = y2 + late * c * (1 - 2 * y2)
        xt = x2 + late * (1 - c) * (1 - 2 * x2)
        return zt, yt, xt

    def send_partner(m, first, k, place):
        zt, yt, xt = place
        return pass_on(m, first, zt, yt, xt, ps.at[m, k], prsem.at[m, ident(zt, yt, xt)], partner)

    def spread_z(m):
        loop(4, lambda k: z_copy(m, k).start(), 1)

    def stage_own(m):
        send_one(m, True, 0).start()
        send_two(m, True, 0).start()
        send_partner(m, True, 0, (z, y, x)).start()
        put_own(m)

    def stage_one(m):
        def body(k):
            zt = lax.rem(z + k, 4)
            arrived(m, zt, y, x)
            send_one(m, False, k).start()
            send_two(m, False, k).start()
            send_partner(m, False, k, (zt, y, x)).start()

        loop(4, body, 1)

    def stage_two(m):
        def body(k):
            zt = lax.rem(z + k, 4)
            arrived(m, zt, y1, x1)
            send_two_late(m, k).start()
            send_partner(m, False, 4 + k, (zt, y1, x1)).start()

        loop(4, body)

    def stage_three(m):
        def body(k):
            place = far_place(k)
            arrived(m, *place)
            send_partner(m, False, 8 + k, place).start()

        loop(8, body)

    def stage_last(m):
        def body(k):
            zt, yt, xt = lax.div(k, 4), lax.rem(lax.div(k, 2), 2), lax.rem(k, 2)
            place = shard(w_refs[m], m, zt, yt, 1 - c, xt)
            remote(place, place, zs.at[m, 0], prsem.at[m, k], partner).wait_recv()

        loop(16, body)

    def drain_weights(m):
        loop(4, lambda k: z_copy(m, k).wait_send(), 1)
        send_one(m, True, 0).wait_send()
        send_two(m, True, 0).wait_send()
        send_partner(m, True, 0, (z, y, x)).wait_send()

        def body(k):
            send_one(m, False, k).wait_send()
            send_two(m, False, k).wait_send()
            send_partner(m, False, k, (lax.rem(z + k, 4), y, x)).wait_send()

        loop(4, body, 1)

        def late(k):
            send_two_late(m, k).wait_send()
            send_partner(m, False, 4 + k, (lax.rem(z + k, 4), y1, x1)).wait_send()

        loop(4, late)
        loop(8, lambda k: send_partner(m, False, 8 + k, far_place(k)).wait_send())

    def c_target(h):
        return lax.rem(x + h, 2)

    def c_copy(h):
        return remote(
            cot.at[pl.ds(h * QUARTER, QUARTER), :],
            G.at[rows_at(x * QUARTER, QUARTER, QUARTER), :],
            c_s.at[h],
            c_r.at[x],
            dev(z, y, c_target(h), c),
        )

    def c_local(h):
        return pltpu.make_async_copy(
            cot.at[pl.ds(h * QUARTER, QUARTER), :],
            G.at[rows_at(x * QUARTER, QUARTER, QUARTER), :],
            c_r.at[x],
        )

    def c_mine(h):
        return jnp.logical_and(c_target(h) == c, x == c)

    spread_z(QKV)
    stage_own(QKV)
    spread_z(PROJ)
    stage_own(PROJ)
    spread_z(UP)
    stage_own(UP)
    for h in (0, 1):

        @pl.when(c_mine(h))
        def _(h=h):
            c_local(h).start()

        @pl.when(jnp.logical_not(c_mine(h)))
        def _(h=h):
            c_copy(h).start()

    spread_z(DOWN)
    stage_own(DOWN)

    stage_one(QKV)

    def v_in(k):
        to = lax.rem(dp + k, 16)
        remote(vec_in, VEC.at[to], v_s.at[0], v_r.at[to], (to, x)).wait_recv()

    loop(16, v_in, 1)

    def lane_parts(width, lanes, shift):
        lane = lax.broadcasted_iota(jnp.int32, (128, lanes), 1).astype(F32)
        part = jnp.floor((lane + 0.5) * (1.0 / width))
        row = lax.broadcasted_iota(jnp.int32, (128, lanes), 0).astype(F32)
        return jnp.where(lane - part * width == row + shift, 1.0, 0.0)

    def lane_owner(width, lanes):
        lane = lax.broadcasted_iota(jnp.int32, (16, lanes), 1)
        first = lax.broadcasted_iota(jnp.int32, (16, lanes), 0) * width
        return jnp.logical_and(lane >= first, lane < first + width)

    pick = lane_parts(48, WIDE, 0.0)
    owner = lane_owner(48, WIDE)
    row_in_48 = lax.broadcasted_iota(jnp.int32, (16, 128), 1) < 48
    for v in range(6):
        part = jnp.where(row_in_48, VEC[:, v, :], 0.0).astype(BF16)
        VF[pl.ds(v, 1), pl.ds(0, WIDE)] = jnp.sum(
            jnp.where(owner, dot_nn(part, pick.astype(BF16)), 0.0), axis=0, keepdims=True
        )

    def wide_vector(j):
        at = rows_at(j * WIDE, WIDE, 128)
        lane = lax.broadcasted_iota(jnp.int32, (128, WIDE), 1).astype(F32)
        lane = lane - 192.0 * jnp.floor((lane + 0.5) * (1.0 / 192.0))
        row = lax.broadcasted_iota(jnp.int32, (128, WIDE), 0).astype(F32)
        low_part = jnp.where(lane == row, 1.0, 0.0)
        high_part = jnp.where(lane == row + 128.0, 1.0, 0.0)
        first = lax.broadcasted_iota(jnp.int32, (16, WIDE), 0) * 192 - j * WIDE
        place = lax.broadcasted_iota(jnp.int32, (16, WIDE), 1)
        held = jnp.logical_and(place >= first, place < first + 192)
        return at, low_part, high_part, held

    for j in range(4):
        at, low_part, high_part, held = wide_vector(j)
        spread = dot_nn(VEC[:, 6, :].astype(BF16), low_part.astype(BF16)) + dot_nn(
            VEC[:, 7, :].astype(BF16), high_part.astype(BF16)
        )
        VF[pl.ds(BU, 1), at] = jnp.sum(jnp.where(held, spread, 0.0), axis=0, keepdims=True)

    def vector(v, at=0, lanes=WIDE):
        return VF[pl.ds(v, 1), pl.ds(at, lanes)]

    def x_in(k):
        place = X.at[rows_at(k * PIECE, PIECE, PIECE), :]
        remote(place, place, x_s.at[0], x_r.at[k], partner).wait_recv()

    loop(16, x_in)

    def norm_parts(values):
        centered = values - jnp.mean(values, axis=-1, keepdims=True)
        spread = jnp.mean(centered * centered, axis=-1, keepdims=True)
        scale = lax.rsqrt(spread + EPSILON)
        return centered * scale, scale

    TILE = 128

    def norm_one(i):
        at = rows_at(i * TILE, TILE, TILE)
        normal, _ = norm_parts(X[at, :].astype(F32))
        A1[at, :] = (normal * vector(G1) + vector(C1)).astype(BF16)

    loop(ROWS // TILE, norm_one)

    stage_two(QKV)
    stage_one(PROJ)
    stage_three(QKV)
    stage_last(QKV)

    def mixed(j):
        at = rows_at(j * QUARTER, QUARTER, QUARTER)
        M[:, at] = dot_nt(A1[...], wq[at, :]).astype(BF16)

    loop(9, mixed, 3)
    kv_copy = remote(M.at[:, pl.ds(WIDE, 2 * WIDE)], KVP, kv_s, kv_r, partner)
    kv_copy.start()
    stage_two(PROJ)
    stage_one(UP)
    loop(3, mixed)
    stage_three(PROJ)
    kv_copy.wait_recv()

    lane_half = lax.broadcasted_iota(jnp.int32, (1, 128), 1) < 64
    offset = lax.broadcasted_iota(jnp.int32, (QUARTER, QUARTER), 1) - lax.broadcasted_iota(
        jnp.int32, (QUARTER, QUARTER), 0
    )
    own_pos = (c * QUARTER, (3 - c) * QUARTER)
    far_pos = ((1 - c) * QUARTER, (2 + c) * QUARTER)

    def head_lanes(values, e):
        keep = lane_half if e == 0 else jnp.logical_not(lane_half)
        return jnp.where(keep, values, jnp.zeros_like(values))

    def masked(scores, key_pos, query_pos):
        return jnp.where(offset >= key_pos - query_pos, scores, NEG_BIG)

    def scores_of(keys, queries, places, qpos):
        return [
            masked(dot_nt(keys[i * QUARTER : (i + 1) * QUARTER], queries), places[i], qpos)
            for i in range(keys.shape[0] // QUARTER)
        ]

    def pair_refs(h):
        at = [rows_at(part * WIDE + h * 128, 128, 128) for part in range(3)]
        return (
            M[:, at[0]],
            M[:, at[1]],
            M[:, at[2]],
            KVP[:, at[0]],
            KVP[:, at[1]],
        )

    def attend_pair(h):
        q2, k_own, v_own, k_far, v_far = pair_refs(h)
        vt_own, vt_far = v_own.T, v_far.T
        pieces = [[None, None], [None, None]]
        for e in (0, 1):
            qm = head_lanes(q2, e) * jnp.asarray(0.125, BF16)
            for b in (0, 1):
                span = QUARTER * (b + 1)
                qs = qm[b * QUARTER : (b + 1) * QUARTER]
                blocks = scores_of(k_own[:span], qs, own_pos, own_pos[b]) + scores_of(
                    k_far[:span], qs, far_pos, own_pos[b]
                )
                top = functools.reduce(
                    jnp.maximum, [jnp.max(s, axis=0, keepdims=True) for s in blocks]
                )
                exps = [jnp.exp(s - top) for s in blocks]
                total = functools.reduce(
                    jnp.add, [jnp.sum(p, axis=0, keepdims=True) for p in exps]
                )
                half = len(exps) // 2
                low_exps = [p.astype(BF16) for p in exps]
                own_w = jnp.concatenate(low_exps[:half], axis=0) if half > 1 else low_exps[0]
                far_w = jnp.concatenate(low_exps[half:], axis=0) if half > 1 else low_exps[1]
                sel = slice(e * 64, (e + 1) * 64)
                mixed_t = dot_nn(vt_own[sel, :span], own_w) + dot_nn(vt_far[sel, :span], far_w)
                pieces[b][e] = mixed_t / total
                LSE[h * 4 + e * 2 + b] = top + jnp.log(total)
        at = rows_at(h * 128, 128, 128)
        for b in (0, 1):
            O[pl.ds(b * QUARTER, QUARTER), at] = (
                jnp.concatenate(pieces[b], axis=0).T.astype(BF16)
            )

    fwd_ticks = [
        lambda: stage_two(UP),
        lambda: stage_one(DOWN),
        lambda: stage_three(UP),
        lambda: stage_two(DOWN),
    ]

    def attend_step(h):
        attend_pair(h)
        for i, tick in enumerate(fwd_ticks):
            pl.when(h == i + 1)(tick)

    loop(6, attend_step)

    stage_last(PROJ)

    def project(j):
        at = rows_at(j * QUARTER, QUARTER, QUARTER)
        R[:, at] = (
            X[:, at].astype(F32) + dot_nt(O[...], wp[at, :]) + VF[pl.ds(BP, 1), at]
        )

    loop(3, project)

    def norm_two(i):
        at = rows_at(i * TILE, TILE, TILE)
        normal, _ = norm_parts(R[at, :])
        A2[at, :] = (normal * vector(G2) + vector(C2)).astype(BF16)

    loop(ROWS // TILE, norm_two)
    stage_last(UP)

    def feed_up(j):
        at = rows_at(j * QUARTER, QUARTER, QUARTER)
        u = dot_nt(A2[...], wu[at, :]) + VF[pl.ds(BU, 1), at]
        square = u * u
        bent = jnp.tanh(TANH_SCALE * (u + CUBIC_TERM * square * u))
        half = 0.5 * (1.0 + bent)
        HD[:, at] = (u * half).astype(BF16)
        slope = half + 0.5 * u * (1.0 - bent * bent) * (
            TANH_SCALE + (3.0 * CUBIC_TERM * TANH_SCALE) * square
        )
        DU[:, at] = slope.astype(BF16)

    loop(12, feed_up)
    stage_three(DOWN)
    stage_last(DOWN)

    length = length_ref[0]

    def live(at_row, count):
        block = lax.div(at_row, QUARTER)
        base = own_pos[0] + block * (own_pos[1] - own_pos[0]) + lax.rem(at_row, QUARTER)
        return lax.broadcasted_iota(jnp.int32, (count, 1), 0) + base < length

    live_rows = jnp.concatenate([live(0, QUARTER), live(QUARTER, QUARTER)], axis=0)

    def feed_down(j):
        at = rows_at(j * QUARTER, QUARTER, QUARTER)
        result = R[:, at] + dot_nt(HD[...], wd[at, :]) + VF[pl.ds(BD, 1), at]
        DRR[:, at] = jnp.where(live_rows, result, 0.0).astype(BF16)

    loop(3, feed_down)

    def o_copy(b):
        return remote(
            DRR.at[pl.ds(b * QUARTER, QUARTER), :],
            out_ref.at[rows_at((c + b - 2 * b * c) * QUARTER, QUARTER, QUARTER), :],
            o_s.at[b],
            o_r.at[c],
            dev(z, y, x, b),
        )

    def o_local(b):
        return pltpu.make_async_copy(
            DRR.at[pl.ds(b * QUARTER, QUARTER), :],
            out_ref.at[rows_at((c + b - 2 * b * c) * QUARTER, QUARTER, QUARTER), :],
            o_s.at[b],
        )

    def o_mine(b):
        return jnp.logical_and(x == c, x == b)

    for b in (0, 1):

        @pl.when(o_mine(b))
        def _(b=b):
            o_local(b).start()

        @pl.when(jnp.logical_not(o_mine(b)))
        def _(b=b):
            o_copy(b).start()

    def r0_copy(m, k):
        n, lanes = SHARDS[m]
        return remote(
            grads[m].at[rows_at((k * 2 + 1 - c) * n, n, 16), :],
            r0_refs[m].at[k],
            r0s.at[m, k],
            r0r.at[m, k],
            partner,
        )

    def add_in(m, zt, yt, xt, part):
        n, lanes = SHARDS[m]
        at = (rows_at((zt * 4 + yt * 2 + c) * n, n, 16), rows_at(xt * lanes, lanes, 128))
        grads[m][at] = (grads[m][at].astype(F32) + part.astype(F32)).astype(BF16)

    def r1_other(k):
        a = lax.rem(k, 2)
        return lax.div(k, 2), (1 - c) * (1 - y) + c * a, (1 - c) * a + c * (1 - x)

    def r1_kept(k):
        a = lax.rem(k, 2)
        return lax.div(k, 2), (1 - c) * y + c * a, (1 - c) * a + c * x

    def r1_copy(m, k):
        zt, yt, xt = r1_other(k)
        return remote(
            shard(grads[m], m, zt, yt, c, xt),
            r1_refs[m].at[k],
            r1s.at[m, k],
            r1r.at[m, k],
            near_two,
        )

    def r2_copy(m, k):
        return remote(
            shard(grads[m], m, k, y1, c, x1), r2_refs[m].at[k], r2s.at[m, k], r2r.at[m, k], near_one
        )

    def r3_copy(m, k):
        zt = lax.rem(z + k, 4)
        return remote(
            shard(grads[m], m, zt, y, c, x),
            r3_refs[m].at[k],
            r3s.at[m, k],
            r3r.at[m, k],
            dev(zt, y, c, x),
        )

    def reduce_start(m):
        loop(8, lambda k: r0_copy(m, k).start())

    def reduce_core(m):
        n, lanes = SHARDS[m]

        def body(k):
            r0_copy(m, k).wait_recv()
            at = rows_at((k * 2 + c) * n, n, 16)
            grads[m][at, :] = (grads[m][at, :].astype(F32) + r0_refs[m][k].astype(F32)).astype(
                BF16
            )

        def both(k):
            body(k)

        loop(8, both)
        loop(8, lambda k: r1_copy(m, k).start())

    def reduce_two(m):
        def body(k):
            r1_copy(m, k).wait_recv()
            zt, yt, xt = r1_kept(k)
            add_in(m, zt, yt, xt, r1_refs[m][k])

        loop(8, body)
        loop(4, lambda k: r2_copy(m, k).start())

    def reduce_one(m):
        def body(k):
            r2_copy(m, k).wait_recv()
            add_in(m, k, y, x, r2_refs[m][k])

        loop(4, body)
        loop(4, lambda k: r3_copy(m, k).start(), 1)

    def reduce_end(m):
        n, lanes = SHARDS[m]
        loop(4, lambda k: r3_copy(m, k).wait_recv(), 1)
        at = (rows_at(dp * n, n, 16), rows_at(x * lanes, lanes, 128))
        total = grads[m][at].astype(F32)
        for k in (1, 2, 3):
            total = total + r3_refs[m][k].astype(F32)
        g_out[m][...] = total

    def drain_grads(m):
        loop(8, lambda k: r0_copy(m, k).wait_send())
        loop(8, lambda k: r1_copy(m, k).wait_send())
        loop(4, lambda k: r2_copy(m, k).wait_send())
        loop(4, lambda k: r3_copy(m, k).wait_send(), 1)

    for b in (0, 1):
        place = G.at[pl.ds(b * QUARTER, QUARTER), :]
        remote(place, place, c_s.at[0], c_r.at[b], partner).wait_recv()
    G[...] = jnp.where(live_rows, G[...], jnp.zeros_like(G))
    GT[...] = G[...].T
    CS[...] = jnp.zeros_like(CS)
    CS[pl.ds(BD, 1), pl.ds(0, WIDE)] = jnp.sum(G[...].astype(F32), axis=0, keepdims=True)

    def down_back(j):
        at = rows_at(j * QUARTER, QUARTER, QUARTER)
        d_u = (dot_nn(G[...], wd[:, at]) * DU[:, at].astype(F32)).astype(BF16)
        DU[:, at] = d_u
        CS[pl.ds(BU, 1), at] = jnp.sum(d_u.astype(F32), axis=0, keepdims=True)

    loop(12, down_back)
    drain_weights(DOWN)

    def down_grad(j):
        at = rows_at(j * QUARTER, QUARTER, QUARTER)
        wd[:, at] = dot_nn(GT[...], HD[:, at]).astype(BF16)

    loop(12, down_grad)
    reduce_start(DOWN)

    def up_back(j):
        at = rows_at(j * QUARTER, QUARTER, QUARTER)
        T1[:, at] = dot_nn(DU[...], wu[:, at])

    loop(3, up_back)
    drain_weights(UP)
    reduce_core(DOWN)

    def up_grad(j):
        at = rows_at(j * QUARTER, QUARTER, QUARTER)
        wu[at, :] = dot_tn(DU[:, at], A2[...]).astype(BF16)

    loop(12, up_grad)
    reduce_start(UP)

    for b in (0, 1):

        @pl.when(o_mine(b))
        def _(b=b):
            o_local(b).wait()

        @pl.when(jnp.logical_not(o_mine(b)))
        def _(b=b):
            o_copy(b).wait_send()

    def add_rows(v, values):
        CS[pl.ds(v, 1), pl.ds(0, WIDE)] += jnp.sum(values, axis=0, keepdims=True)

    def norm_two_back(i):
        at = rows_at(i * TILE, TILE, TILE)
        normal, scale = norm_parts(R[at, :])
        d_a = T1[at, :]
        e = d_a * vector(G2)
        inner = (
            e
            - jnp.mean(e, axis=-1, keepdims=True)
            - normal * jnp.mean(e * normal, axis=-1, keepdims=True)
        )
        d_r = G[at, :].astype(F32) + inner * scale
        T1[at, :] = d_r
        DRR[at, :] = d_r.astype(BF16)
        add_rows(G2, d_a * normal)
        add_rows(C2, d_a)
        add_rows(BP, d_r)

    loop(ROWS // TILE, norm_two_back)
    reduce_core(UP)
    reduce_two(DOWN)

    def project_back(j):
        at = rows_at(j * QUARTER, QUARTER, QUARTER)
        A2[:, at] = dot_nn(DRR[...], wp[:, at]).astype(BF16)

    loop(3, project_back)
    drain_weights(PROJ)

    def project_grad(j):
        at = rows_at(j * QUARTER, QUARTER, QUARTER)
        wp[at, :] = dot_tn(DRR[:, at], O[...]).astype(BF16)

    loop(3, project_grad)
    reduce_start(PROJ)
    kv_copy.wait_send()

    def dk_copy(h, part):
        at = rows_at(part * WIDE + h * 128, 128, 128)
        return remote(DKVP.at[:, at], RK.at[:, at], dk_s.at[h, part], dk_r.at[h, part], partner)

    def attend_back(h):
        q2, k_own, v_own, k_far, v_far = pair_refs(h)
        do2 = A2[:, rows_at(h * 128, 128, 128)]
        kt_own, kt_far = k_own.T, k_far.T
        dq = [[None, None], [None, None]]
        d_keys = [None] * 4
        d_vals = [None] * 4

        def gather(store, i, value):
            store[i] = value if store[i] is None else store[i] + value

        for e in (0, 1):
            qm = head_lanes(q2, e) * jnp.asarray(0.125, BF16)
            dom = head_lanes(do2, e)
            for b in (0, 1):
                span = QUARTER * (b + 1)
                rows = slice(b * QUARTER, (b + 1) * QUARTER)
                qs, dos = qm[rows], dom[rows]
                log_total = LSE[h * 4 + e * 2 + b]
                blocks = scores_of(k_own[:span], qs, own_pos, own_pos[b]) + scores_of(
                    k_far[:span], qs, far_pos, own_pos[b]
                )
                weights = [jnp.exp(s - log_total) for s in blocks]
                values = [v_own[i * QUARTER : (i + 1) * QUARTER] for i in range(b + 1)] + [
                    v_far[i * QUARTER : (i + 1) * QUARTER] for i in range(b + 1)
                ]
                d_w = [dot_nt(v, dos) for v in values]
                delta = functools.reduce(
                    jnp.add,
                    [jnp.sum(p * d, axis=0, keepdims=True) for p, d in zip(weights, d_w)],
                )
                d_s = [(p * (d - delta)).astype(BF16) for p, d in zip(weights, d_w)]
                sel = slice(e * 64, (e + 1) * 64)
                total = None
                for i, d in enumerate(d_s):
                    kt = kt_own if i <= b else kt_far
                    j = i if i <= b else i - b - 1
                    term = dot_nn(kt[sel, j * QUARTER : (j + 1) * QUARTER], d)
                    total = term if total is None else total + term
                    where = j if i <= b else 2 + j
                    gather(d_keys, where, dot_nn(d, qs))
                    gather(d_vals, where, dot_nn(weights[i].astype(BF16), dos))
                dq[b][e] = total * 0.125
        for b in (0, 1):
            M[pl.ds(b * QUARTER, QUARTER), rows_at(h * 128, 128, 128)] = (
                jnp.concatenate(dq[b], axis=0).T.astype(BF16)
            )
        for part, store in ((0, d_keys), (1, d_vals)):
            for i in (0, 1):
                rows = pl.ds(i * QUARTER, QUARTER)
                M[rows, rows_at((1 + part) * WIDE + h * 128, 128, 128)] = store[i].astype(BF16)
                DKVP[rows, rows_at(part * WIDE + h * 128, 128, 128)] = store[2 + i].astype(BF16)
        for part in (0, 1):
            dk_copy(h, part).start()

    bwd_ticks = [
        lambda: reduce_core(PROJ),
        lambda: reduce_two(UP),
        lambda: reduce_one(DOWN),
        lambda: reduce_two(PROJ),
        lambda: reduce_one(UP),
    ]

    def attend_back_step(h):
        attend_back(h)
        for i, tick in enumerate(bwd_ticks):
            pl.when(h == i)(tick)

    loop(6, attend_back_step)

    def settle(h):
        for part in (0, 1):
            dk_copy(h, part).wait_recv()
            at = rows_at((1 + part) * WIDE + h * 128, 128, 128)
            M[:, at] = (
                M[:, at].astype(F32) + RK[:, rows_at(part * WIDE + h * 128, 128, 128)].astype(F32)
            ).astype(BF16)

    loop(6, settle)

    def qkv_grad(j):
        at = rows_at(j * QUARTER, QUARTER, QUARTER)
        gq[at, :] = dot_tn(M[:, at], A1[...]).astype(BF16)

    loop(9, qkv_grad)
    reduce_start(QKV)
    reduce_one(PROJ)

    grad_first = R

    def qkv_back(j):
        at = rows_at(j * QUARTER, QUARTER, QUARTER)
        grad_first[:, at] = dot_nn(M[...], wq[:, at])

    loop(3, qkv_back)
    reduce_core(QKV)

    def norm_one_back(i):
        at = rows_at(i * TILE, TILE, TILE)
        normal, scale = norm_parts(X[at, :].astype(F32))
        d_a = grad_first[at, :]
        e = d_a * vector(G1)
        inner = (
            e
            - jnp.mean(e, axis=-1, keepdims=True)
            - normal * jnp.mean(e * normal, axis=-1, keepdims=True)
        )
        A2[at, :] = (T1[at, :] + inner * scale).astype(BF16)
        add_rows(G1, d_a * normal)
        add_rows(C1, d_a)

    loop(ROWS // TILE, norm_one_back)

    def ret_place(k):
        b, r = lax.div(k, 8), lax.rem(k, 8)
        zt = 2 * lax.rem(c + b, 2) + lax.div(r, 4)
        return zt, lax.rem(lax.div(r, 2), 2), lax.rem(r, 2), b

    def ret_copy(k):
        return remote(
            A2.at[rows_at(k * PIECE, PIECE, PIECE), :],
            ret_ref.at[slot],
            ret_s.at[k],
            ret_r.at[slot],
            dev(*ret_place(k)),
        )

    def ret_local(k):
        return pltpu.make_async_copy(
            A2.at[rows_at(k * PIECE, PIECE, PIECE), :], ret_ref.at[slot], ret_s.at[k]
        )

    def ret_mine(k):
        zt, yt, ct, xt = ret_place(k)
        return (zt * 4 + yt * 2 + ct) * 2 + xt == me

    def ret_start(k):
        pl.when(ret_mine(k))(lambda: ret_local(k).start())
        pl.when(jnp.logical_not(ret_mine(k)))(lambda: ret_copy(k).start())

    def ret_end(k):
        pl.when(ret_mine(k))(lambda: ret_local(k).wait())
        pl.when(jnp.logical_not(ret_mine(k)))(lambda: ret_copy(k).wait_send())

    loop(16, ret_start)

    highest = lax.Precision.HIGHEST
    for v in range(6):
        spread = jnp.where(owner, CS[pl.ds(v, 1), pl.ds(0, WIDE)], 0.0)
        VGS[:, v, :] = lax.dot_general(
            spread, pick, (((1,), (1,)), ((), ())), precision=highest, preferred_element_type=F32
        )
    lows, highs = (None, None)
    for j in range(4):
        at, low_part, high_part, held = wide_vector(j)
        spread = jnp.where(held, CS[pl.ds(BU, 1), at], 0.0)
        a = lax.dot_general(
            spread, low_part, (((1,), (1,)), ((), ())), precision=highest, preferred_element_type=F32
        )
        b = lax.dot_general(
            spread, high_part, (((1,), (1,)), ((), ())), precision=highest, preferred_element_type=F32
        )
        lows, highs = (a, b) if lows is None else (lows + a, highs + b)
    VGS[:, 6, :] = lows
    VGS[:, 7, :] = highs

    def vg_copy(k):
        other = lax.rem(me + k, 32)
        to = lax.div(other, 2)
        return remote(
            VGS.at[to], VGR.at[me], vg_s.at[k], vg_r.at[me], (to, lax.rem(other, 2))
        )

    def vg_in(k):
        other = lax.rem(me + k, 32)
        remote(VGS.at[0], VGR.at[other], vg_s.at[0], vg_r.at[other], partner).wait_recv()

    loop(32, lambda k: vg_copy(k).start(), 1)
    VGR[pl.ds(me, 1)] = VGS[pl.ds(dp, 1)]

    reduce_two(QKV)
    reduce_one(QKV)
    for m in (DOWN, UP, PROJ):
        reduce_end(m)
    loop(32, vg_in, 1)
    gvec_out[...] = jnp.sum(VGR[...], axis=0)
    reduce_end(QKV)

    def ret_in(k):
        remote(A2.at[pl.ds(0, PIECE), :], ret_ref.at[k], ret_s.at[0], ret_r.at[k], partner).wait_recv()

    def ret_wait(k):
        stays = jnp.logical_and(k == slot, x_mine)
        pl.when(jnp.logical_not(stays))(lambda: ret_in(k))

    loop(16, ret_wait)

    def o_in(b):
        place = out_ref.at[pl.ds(0, QUARTER), :]
        remote(place, place, o_s.at[0], o_r.at[b], partner).wait_recv()

    for b in (0, 1):
        stays = jnp.logical_and(x == c, c == b)
        pl.when(jnp.logical_not(stays))(functools.partial(o_in, b))

    pl.when(x_mine)(lambda: None)
    pl.when(jnp.logical_not(x_mine))(lambda: x_copy(0).wait_send())
    loop(16, lambda k: x_copy(k).wait_send(), 1)
    loop(16, lambda k: v_copy(k).wait_send(), 1)
    for h in (0, 1):
        pl.when(jnp.logical_not(c_mine(h)))(functools.partial(lambda h: c_copy(h).wait_send(), h))
    drain_weights(QKV)
    for m in range(4):
        drain_grads(m)

    def dk_end(h):
        for part in (0, 1):
            dk_copy(h, part).wait_send()

    loop(6, dk_end)
    loop(16, ret_end)
    loop(32, lambda k: vg_copy(k).wait_send(), 1)


def block_local(
    x_source,
    cotangent,
    lengths,
    dealing,
    qkv_weight,
    proj_weight,
    up_weight,
    down_weight,
    *vectors,
):
    slots = x_source.shape[0]
    places = jnp.arange(slots, dtype=jnp.int32)
    owners = jnp.sum(jnp.where(dealing[None, :] == places[:, None], places[None, :], 0), axis=1)
    dp = lax.axis_index("dp")
    slot = (dp // 2) * 2 + lax.axis_index("cp")
    length = jnp.sum(jnp.where(dealing == slot, lengths, 0)).reshape(1)
    gathered = x_source[owners]
    first_gain, first_shift, proj_bias, second_gain, second_shift, up_bias, down_bias = vectors
    narrow = [
        jnp.pad(vector, (0, 128 - vector.shape[0]))
        for vector in (first_gain, first_shift, proj_bias, second_gain, second_shift, down_bias)
    ]
    up_rows = jnp.pad(up_bias, (0, 256 - up_bias.shape[0])).reshape(2, 128)
    packed = jnp.concatenate([jnp.stack(narrow), up_rows]).astype(BF16).astype(F32)
    weights = [
        weight.astype(BF16).T for weight in (qkv_weight, proj_weight, up_weight, down_weight)
    ]
    vmem = pl.BlockSpec(memory_space=pltpu.VMEM)
    smem = pl.BlockSpec(memory_space=pltpu.SMEM)
    dma = pltpu.SemaphoreType.DMA

    def act(*shape, dtype=BF16):
        return pltpu.VMEM(shape, dtype)

    full = [act(16 * n, 2 * lanes) for n, lanes in SHARDS]
    acts = (
        act(ROWS, WIDE),
        act(ROWS, WIDE),
        act(ROWS, 3 * WIDE),
        act(ROWS, 2 * WIDE),
        act(ROWS, WIDE),
        act(ROWS, WIDE, dtype=F32),
        act(ROWS, WIDE),
        act(ROWS, HIDDEN),
        act(ROWS, HIDDEN),
        act(ROWS, WIDE, dtype=F32),
        act(ROWS, WIDE),
        act(ROWS, WIDE),
        act(WIDE, ROWS),
        act(ROWS, 2 * WIDE),
        act(ROWS, 2 * WIDE),
        act(24, 1, QUARTER, dtype=F32),
        act(16, 8, 128, dtype=F32),
        act(8, HIDDEN, dtype=F32),
        act(8, HIDDEN, dtype=F32),
        act(16, 8, 128, dtype=F32),
        act(32, 8, 128, dtype=F32),
    )
    sems = (
        dma((16,)),
        dma((16,)),
        dma((16,)),
        dma((16,)),
        dma((2,)),
        dma((2,)),
        dma((4, 4)),
        dma((4, 4)),
        dma((4, 8)),
        dma((4, 16)),
        dma((4, 16)),
        dma((4, 16)),
        dma,
        dma,
        dma((2,)),
        dma((2,)),
        dma((4, 8)),
        dma((4, 8)),
        dma((4, 8)),
        dma((4, 8)),
        dma((4, 4)),
        dma((4, 4)),
        dma((4, 4)),
        dma((4, 4)),
        dma((6, 2)),
        dma((6, 2)),
        dma((16,)),
        dma((16,)),
        dma((32,)),
        dma((32,)),
    )
    results = pl.pallas_call(
        block_kernel,
        out_shape=(
            jax.ShapeDtypeStruct((ROWS, WIDE), BF16),
            jax.ShapeDtypeStruct((16, PIECE, WIDE), BF16),
            *[jax.ShapeDtypeStruct(shard, F32) for shard in SHARDS],
            jax.ShapeDtypeStruct((8, 128), F32),
        ),
        in_specs=[smem] + [vmem] * 7,
        out_specs=(vmem,) * 7,
        scratch_shapes=[
            *full,
            act(16 * SHARDS[QKV][0], 2 * SHARDS[QKV][1]),
            tuple(act(8, n, 2 * lanes) for n, lanes in SHARDS),
            tuple(act(8, n, lanes) for n, lanes in SHARDS),
            tuple(act(4, n, lanes) for n, lanes in SHARDS),
            tuple(act(4, n, lanes) for n, lanes in SHARDS),
            acts,
            sems,
        ],
        compiler_params=pltpu.CompilerParams(
            collective_id=0, has_side_effects=True, vmem_limit_bytes=67043328
        ),
        name="block_step",
    )(length, gathered, cotangent[0], *weights, packed)
    output, returned, gq, gp, gu, gd, gvec = results
    owned = [gvec[v, : vector.shape[0]] for v, vector in ((G1, first_gain), (C1, first_shift))]
    owned += [gvec[v, : proj_bias.shape[0]] for v in (BP, G2, C2)]
    owned += [gvec[6:8].reshape(-1)[: up_bias.shape[0]], gvec[BD, : down_bias.shape[0]]]
    return (
        output[None],
        returned[dealing],
        gq.T,
        gp.T,
        gu.T,
        gd.T,
        *owned,
    )

def solution(mesh):
    in_specs = (
        P(None, ("cp", "dp"), None),
        P("dp", "cp", None),
        P(),
        P(),
        P("cp", "dp"),
        P("cp", "dp"),
        P("cp", "dp"),
        P("cp", "dp"),
        P("dp"),
        P("dp"),
        P("dp"),
        P("dp"),
        P("dp"),
        P("dp"),
        P("dp"),
    )
    out_specs = (
        P("dp", "cp", None),
        P(None, ("cp", "dp"), None),
        P("cp", "dp"),
        P("cp", "dp"),
        P("cp", "dp"),
        P("cp", "dp"),
        P("dp"),
        P("dp"),
        P("dp"),
        P("dp"),
        P("dp"),
        P("dp"),
        P("dp"),
    )
    step = block_local if fits_block(mesh) else local
    return jax.shard_map(step, mesh=mesh, in_specs=in_specs, out_specs=out_specs, check_vma=False)
```
